32 devices in a mesh: unit: 4 (over y, x), replica: 2 (over core), model: 4 (over z).
Axes of the slice: x: 2, y: 2, z: 4, core: 2. Of those that a mesh axis runs over, the one named last changes fastest.
Arguments:
- slope_up: float32 [8, 768, 3072], P(('unit', 'replica'), None, 'model'), parts along dimension 0, may hold values from -0.875 to 0.875
- slope_down: float32 [8, 3072, 768], P(('unit', 'replica'), 'model'), parts along dimension 0, may hold values from -0.875 to 0.875
- slope_query: float32 [8, 768, 768], P(('unit', 'replica'), None, 'model'), parts along dimension 0, may hold values from -0.875 to 0.875
- slope_key: float32 [8, 768, 768], P(('unit', 'replica'), None, 'model'), parts along dimension 0, may hold values from -0.875 to 0.875
- slope_value: float32 [8, 768, 768], P(('unit', 'replica'), None, 'model'), parts along dimension 0, may hold values from -0.875 to 0.875
- slope_mixed: float32 [8, 768, 768], P(('unit', 'replica'), 'model'), parts along dimension 0, may hold values from -0.875 to 0.875
- slope_norm: float32 [8, 768], P(('unit', 'replica')), parts along dimension 0, may hold values from -8 to 8
- param_up: float32 [3072, 3072], P(('unit', 'replica'), 'model'), parts along dimension 0, may hold values from -0.21875 to 0.21875
- param_down: float32 [12288, 768], P(('unit', 'model'), 'replica'), parts along dimension 0, may hold values from -0.109375 to 0.109375
- param_query: float32 [3072, 768], P(('unit', 'replica'), 'model'), parts along dimension 0, may hold values from -0.21875 to 0.21875
- param_key: float32 [3072, 768], P(('unit', 'replica'), 'model'), parts along dimension 0, may hold values from -0.21875 to 0.21875
- param_value: float32 [3072, 768], P(('unit', 'replica'), 'model'), parts along dimension 0, may hold values from -0.21875 to 0.21875
- param_mixed: float32 [3072, 768], P(('unit', 'model'), 'replica'), parts along dimension 0, may hold values from -0.21875 to 0.21875
- param_norm: float32 [3072], P(('unit', 'replica')), parts along dimension 0, may hold values from 0.25 to 1.75
Outputs:
- half_up: bfloat16 [3072, 3072], P('unit', 'model'), parts along dimension 0
- half_down: bfloat16 [12288, 768], P(('unit', 'model')), parts along dimension 0
- half_query: bfloat16 [3072, 768], P('unit', 'model'), parts along dimension 0
- half_key: bfloat16 [3072, 768], P('unit', 'model'), parts along dimension 0
- half_value: bfloat16 [3072, 768], P('unit', 'model'), parts along dimension 0
- half_mixed: bfloat16 [3072, 768], P(('unit', 'model')), parts along dimension 0
- half_norm: bfloat16 [3072], P('unit'), parts along dimension 0
- next_up: float32 [3072, 3072], P(('unit', 'replica'), 'model'), parts along dimension 0
- next_down: float32 [12288, 768], P(('unit', 'model'), 'replica'), parts along dimension 0
- next_query: float32 [3072, 768], P(('unit', 'replica'), 'model'), parts along dimension 0
- next_key: float32 [3072, 768], P(('unit', 'replica'), 'model'), parts along dimension 0
- next_value: float32 [3072, 768], P(('unit', 'replica'), 'model'), parts along dimension 0
- next_mixed: float32 [3072, 768], P(('unit', 'model'), 'replica'), parts along dimension 0
- next_norm: float32 [3072], P(('unit', 'replica')), parts along dimension 0
The draws below stay inside these ranges and needn't reach their ends.
There are 4 independent parts, one for each index of `unit`. The reference program is written for one: setup_inputs(seed, part) draws one part's arguments, and reference() takes and returns one part's arrays. A program takes and returns all parts, laid end to end along the dimension named above; each array names one. Nothing has to cross between parts.
All inputs are finite; a program needn't handle non-finite values.
Results may differ from the reference program's by a relative error of at most 0.001.
Values may be sent and summed in bfloat16 or wider, within the bound.
A program may use at most 64 MiB of HBM per device.

```python
import jax
import jax.numpy as jnp

WIDTH = 768
INNER = 3072
ATTN = 768
REPLICAS = 2


def spiked(array, stream_key, source, target, shards_of, factor):
    owner, partner = [(jnp.arange(array.shape[axis_at]) // (array.shape[axis_at] // shards_of)).reshape([-1 if axis == axis_at else 1 for axis in range(array.ndim)]) for axis_at in (source, target)]
    chosen = jax.random.permutation(stream_key, shards_of)[partner]
    strong = (owner == chosen) | (owner == (partner + shards_of // 2) % shards_of)
    return jnp.where(strong, factor * array, array)


def block_levels(key, shape, split, low, largest):
    gain, own = 1.0, jax.random.fold_in(key, 6)
    for axis_at, parts in split:
        heights = jnp.exp(jax.random.uniform(jax.random.fold_in(own, axis_at), (parts,), jnp.float32, low / len(split), largest / len(split)))
        gain = gain * jnp.repeat(heights, shape[axis_at] // parts).reshape([-1 if axis == axis_at else 1 for axis in range(len(shape))])
    return gain


def centred(stream_key, extent, deviation, reach, split=(), kind=jnp.bfloat16):
    entries = deviation * jax.random.normal(stream_key, extent, jnp.float32)
    if split:
        entries = entries * block_levels(stream_key, extent, split, -0.22, 0.18)
    return jnp.clip(entries, -reach, reach).astype(kind)


def noise_with(stream_key, dims, scale, most, pieces, heavy, dtype=jnp.bfloat16):
    values = scale * jax.random.normal(stream_key, dims, jnp.float32)
    if pieces:
        values = values * block_levels(stream_key, dims, pieces, -0.22, 0.18)
    return jnp.clip(spiked(values, jax.random.fold_in(stream_key, 3), *heavy), -most, most).astype(dtype)


def setup_inputs(seed: int = 0, part: int = 0) -> dict:
    streams_of = jax.random.split(jax.random.key(seed), 15)
    part_keys = jax.random.split(jax.random.fold_in(streams_of[14], part), 15)
    return {
        "slope_up": noise_with(part_keys[0], (REPLICAS, WIDTH, INNER), 0.1, 0.875, ((0, 2), (2, 4)), (0, 1, 2, 2.0), jnp.float32),
        "slope_down": noise_with(part_keys[1], (REPLICAS, INNER, WIDTH), 0.1, 0.875, ((0, 2), (1, 4)), (0, 2, 2, 2.0), jnp.float32),
        "slope_query": noise_with(part_keys[2], (REPLICAS, WIDTH, ATTN), 0.1, 0.875, ((0, 2), (2, 4)), (0, 1, 2, 2.0), jnp.float32),
        "slope_key": noise_with(part_keys[3], (REPLICAS, WIDTH, ATTN), 0.1, 0.875, ((0, 2), (2, 4)), (0, 1, 2, 2.0), jnp.float32),
        "slope_value": noise_with(part_keys[4], (REPLICAS, WIDTH, ATTN), 0.1, 0.875, ((0, 2), (2, 4)), (0, 1, 2, 2.0), jnp.float32),
        "slope_mixed": noise_with(part_keys[5], (REPLICAS, ATTN, WIDTH), 0.1, 0.875, ((0, 2), (1, 4)), (0, 2, 2, 2.0), jnp.float32),
        "slope_norm": noise_with(part_keys[6], (REPLICAS, WIDTH), 1.0, 8.0, ((0, 2),), (0, 1, 2, 2.0), jnp.float32),
        "param_up": centred(part_keys[7], (WIDTH, INNER), WIDTH ** -0.5, 0.21875, ((0, 2), (1, 4)), jnp.float32),
        "param_down": centred(part_keys[8], (INNER, WIDTH), INNER ** -0.5, 0.109375, ((0, 4), (1, 2)), jnp.float32),
        "param_query": centred(part_keys[9], (WIDTH, ATTN), WIDTH ** -0.5, 0.21875, ((0, 2), (1, 4)), jnp.float32),
        "param_key": centred(part_keys[10], (WIDTH, ATTN), WIDTH ** -0.5, 0.21875, ((0, 2), (1, 4)), jnp.float32),
        "param_value": centred(part_keys[11], (WIDTH, ATTN), WIDTH ** -0.5, 0.21875, ((0, 2), (1, 4)), jnp.float32),
        "param_mixed": centred(part_keys[12], (ATTN, WIDTH), ATTN ** -0.5, 0.21875, ((0, 4), (1, 2)), jnp.float32),
        "param_norm": jnp.clip(1.0 + 0.15 * jax.random.normal(part_keys[13], (WIDTH,), jnp.float32), 0.25, 1.75),
    }


learn_rate = 0.3


def reference(slope_up, slope_down, slope_query, slope_key, slope_value, slope_mixed, slope_norm, param_up, param_down, param_query, param_key, param_value, param_mixed, param_norm):
    mean_up = jnp.sum(slope_up.astype(jnp.float32), axis=0) * REPLICAS ** -0.5
    mean_down = jnp.sum(slope_down.astype(jnp.float32), axis=0) * REPLICAS ** -0.5
    mean_query = jnp.sum(slope_query.astype(jnp.float32), axis=0) * REPLICAS ** -0.5
    mean_key = jnp.sum(slope_key.astype(jnp.float32), axis=0) * REPLICAS ** -0.5
    mean_value = jnp.sum(slope_value.astype(jnp.float32), axis=0) * REPLICAS ** -0.5
    mean_mixed = jnp.sum(slope_mixed.astype(jnp.float32), axis=0) * REPLICAS ** -0.5
    mean_norm = jnp.sum(slope_norm.astype(jnp.float32), axis=0) * REPLICAS ** -0.5
    next_up = param_up - learn_rate * mean_up
    next_down = param_down - learn_rate * mean_down
    next_query = param_query - learn_rate * mean_query
    next_key = param_key - learn_rate * mean_key
    next_value = param_value - learn_rate * mean_value
    next_mixed = param_mixed - learn_rate * mean_mixed
    next_norm = param_norm - learn_rate * mean_norm
    half_up = next_up.astype(jnp.bfloat16)
    half_down = next_down.astype(jnp.bfloat16)
    half_query = next_query.astype(jnp.bfloat16)
    half_key = next_key.astype(jnp.bfloat16)
    half_value = next_value.astype(jnp.bfloat16)
    half_mixed = next_mixed.astype(jnp.bfloat16)
    half_norm = next_norm.astype(jnp.bfloat16)
    return half_up, half_down, half_query, half_key, half_value, half_mixed, half_norm, next_up, next_down, next_query, next_key, next_value, next_mixed, next_norm
```

```python
import functools

import jax
import jax.numpy as jnp
from jax import lax
from jax.experimental import pallas as pl
from jax.experimental.pallas import tpu as pltpu
from jax.sharding import PartitionSpec as P

learn_rate = 0.3
ANY = pl.BlockSpec(memory_space=pl.ANY)
VMEM_BYTES = 67043328


def pieces(shape, split_rows, parts):
    rows = shape[0]
    if rows % (16 * parts):
        parts = 1
    return [(part * (rows // parts), rows // parts) for part in range(parts)]


def plan(halves, by_row, small):
    chunks = []
    for at, half in enumerate(halves):
        parts = max(1, half[0] * half[1] // small)
        chunks += [(at, start, rows) for start, rows in pieces(half, by_row[at], parts)]
    return chunks


def exchange(n, by_row, chunks, rate, *refs):
    m = len(by_row)
    slopes, slope_norm = refs[:m], refs[m]
    params, param_norm = refs[m + 1 : 2 * m + 1], refs[2 * m + 1]
    refs = refs[2 * m + 2 :]
    halfs, norm_half = refs[:m], refs[m]
    kept, norm_next = refs[m + 1 : 2 * m + 1], refs[2 * m + 1]
    refs = refs[2 * m + 2 :]
    own, got = refs[:m], refs[m : 2 * m]
    (norms, norm_kept, in_sem, keep_sem, send_sem, recv_sem,
     back_send, back_recv, norm_in, norm_send, norm_recv) = refs[2 * m :]

    me = lax.axis_index("replica")
    peer = 1 - me
    there = {"replica": peer}

    def half_of(at, who, start, rows):
        height, width = kept[at].shape
        if by_row[at]:
            return pl.ds(pl.multiple_of(who * height + start, 16), rows), pl.ds(0, width)
        return pl.ds(start, rows), pl.ds(pl.multiple_of(who * width, width), width)

    def remote(source, target, out_sem, in_sem):
        return pltpu.make_async_remote_copy(
            src_ref=source,
            dst_ref=target,
            send_sem=out_sem,
            recv_sem=in_sem,
            device_id=there,
            device_id_type=pl.DeviceIdType.MESH,
        )

    loads = []
    for c, (at, start, rows) in enumerate(chunks):
        mine = pl.ds(start, rows)
        loads.append((
            pltpu.make_async_copy(
                slopes[at].at[(0, *half_of(at, me, start, rows))], own[at].at[mine], in_sem.at[c]
            ),
            pltpu.make_async_copy(params[at].at[mine], kept[at].at[mine], keep_sem.at[c]),
        ))
    norm_loads = (
        pltpu.make_async_copy(slope_norm, norms.at[pl.ds(me, 1)], norm_in.at[0]),
        pltpu.make_async_copy(param_norm, norm_kept.at[pl.ds(me, 1)], norm_in.at[1]),
    )

    barrier = pltpu.get_barrier_semaphore()
    pl.semaphore_signal(barrier, inc=1, device_id=there, device_id_type=pl.DeviceIdType.MESH)
    pl.semaphore_wait(barrier, 1)

    norm_sends = [
        remote(slope_norm, norms.at[pl.ds(me, 1)], norm_send.at[0], norm_recv.at[0]),
        remote(param_norm, norm_kept.at[pl.ds(me, 1)], norm_send.at[1], norm_recv.at[1]),
    ]
    sends = [
        remote(
            slopes[at].at[(0, *half_of(at, peer, start, rows))],
            got[at].at[pl.ds(start, rows)],
            send_sem.at[c],
            recv_sem.at[c],
        )
        for c, (at, start, rows) in enumerate(chunks)
    ]
    for send in sends + norm_sends:
        send.start()
    for load in loads:
        load[0].start()
        load[1].start()
    for load in norm_loads:
        load.start()

    backs = []
    for c, (at, start, rows) in enumerate(chunks):
        loads[c][0].wait()
        loads[c][1].wait()
        sends[c].wait_recv()
        step = 32 if rows % 32 == 0 else 16
        height, width = kept[at].shape

        @pl.loop(0, rows // step)
        def update(block, at=at, start=start, step=step, height=height, width=width):
            first = pl.multiple_of(start + block * step, step)
            span = pl.ds(first, step)
            mean = (own[at][span] + got[at][span]) * rate
            moved = kept[at][span] - learn_rate * mean
            kept[at][span] = moved
            halfs[at][half_of(at, me, first, step)] = moved.astype(jnp.bfloat16)

        place = half_of(at, me, start, rows)
        back = remote(halfs[at].at[place], halfs[at].at[place], back_send.at[c], back_recv.at[c])
        back.start()
        backs.append(back)

    for load in norm_loads:
        load.wait()
    for send in norm_sends:
        send.wait_recv()
    width = norm_kept.shape[1]
    for who in range(n):
        cut = pl.ds(who * width, width)
        total = norms[0:1, cut]
        for other in range(1, n):
            total += norms[other : other + 1, cut]
        moved = norm_kept[who : who + 1] - learn_rate * (total * rate)
        norm_half[0:1, cut] = moved

        @pl.when(who == me)
        def keep():
            norm_next[...] = moved

    for send in sends + norm_sends:
        send.wait_send()
    for back in backs:
        back.wait()


def settle(count, *refs):
    sems = refs[-1]
    copies = [
        pltpu.make_async_copy(refs[k], refs[count + k], sems.at[k]) for k in range(count)
    ]
    for copy in copies:
        copy.start()
    for copy in copies:
        copy.wait()


def shards(n, *arrays):
    m = len(arrays) // 2 - 1
    slopes, slope_norm = list(arrays[:m]), arrays[m]
    params, param_norm = list(arrays[m + 1 : -1]), arrays[-1]
    turned = [2, 3, 4]
    by_row = [slope.shape[1] != param.shape[0] for slope, param in zip(slopes, params)]
    for at in turned:
        slopes[at] = slopes[at].transpose(0, 2, 1)
        params[at] = params[at].T
        by_row[at] = not by_row[at]
    f32, bf16 = jnp.float32, jnp.bfloat16
    halves = [param.shape for param in params]
    wholes = [slope.shape[1:] for slope in slopes]
    small = min(half[0] * half[1] for half in halves)
    chunks = plan(halves, by_row, small)
    count = len(chunks)
    width = param_norm.shape[0]
    dma = pltpu.SemaphoreType.DMA
    results = sum(rows * columns for rows, columns in wholes) * 2
    results += sum(rows * columns for rows, columns in halves) * 4
    outs = pl.pallas_call(
        functools.partial(exchange, n, by_row, chunks, n ** (-0.5)),
        out_shape=(
            *[pltpu.VMEM(whole, bf16) for whole in wholes],
            pltpu.VMEM((1, n * width), f32),
            *[pltpu.VMEM(half, f32) for half in halves],
            pltpu.VMEM((1, width), f32),
        ),
        in_specs=[ANY] * (2 * m + 2),
        out_specs=[pl.BlockSpec(memory_space=pltpu.VMEM)] * (2 * m + 2),
        scratch_shapes=[
            *[pltpu.VMEM(half, f32) for half in halves * 2],
            pltpu.VMEM((n, n * width), f32),
            pltpu.VMEM((n, width), f32),
            *[dma((count,))] * 6,
            *[dma((2,))] * 3,
        ],
        compiler_params=pltpu.CompilerParams(
            collective_id=0, has_side_effects=True, vmem_limit_bytes=VMEM_BYTES - results - 192 * 1024
        ),
        name="exchange",
    )(*slopes, slope_norm, *params, param_norm.reshape(1, width))
    outs = list(outs)
    norm_half, norm_next = outs.pop(m), outs.pop()
    outs = list(pl.pallas_call(
        functools.partial(settle, 2 * m),
        out_shape=(
            *[jax.ShapeDtypeStruct(whole, bf16) for whole in wholes],
            *[jax.ShapeDtypeStruct(half, f32) for half in halves],
        ),
        in_specs=[pl.BlockSpec(memory_space=pltpu.VMEM)] * (2 * m),
        out_specs=[ANY] * (2 * m),
        scratch_shapes=[dma((2 * m,))],
        compiler_params=pltpu.CompilerParams(vmem_limit_bytes=2 * 1024 * 1024),
        name="settle",
    )(*outs))
    for at in turned:
        outs[at] = outs[at].T
        outs[m + at] = outs[m + at].T
    half_norm = norm_half.reshape(n * width).astype(bf16)
    return (*outs[:m], half_norm, *outs[m:], norm_next.reshape(width))


def spread(
    slope_up,
    slope_down,
    slope_query,
    slope_key,
    slope_value,
    slope_mixed,
    slope_norm,
    param_up,
    param_down,
    param_query,
    param_key,
    param_value,
    param_mixed,
    param_norm,
):
    mean_up, mean_down, mean_query, mean_key, mean_value, mean_mixed = (
        lax.psum_scatter(slope_up[0], "replica", scatter_dimension=0, tiled=True),
        lax.psum_scatter(slope_down[0], "replica", scatter_dimension=1, tiled=True),
        lax.psum_scatter(slope_query[0], "replica", scatter_dimension=0, tiled=True),
        lax.psum_scatter(slope_key[0], "replica", scatter_dimension=0, tiled=True),
        lax.psum_scatter(slope_value[0], "replica", scatter_dimension=0, tiled=True),
        lax.psum_scatter(slope_mixed[0], "replica", scatter_dimension=1, tiled=True),
    )
    whole_norm = lax.psum(slope_norm[0], "replica")
    place = lax.axis_index("replica")
    mean_norm = lax.dynamic_slice_in_dim(
        whole_norm, place * param_norm.shape[0], param_norm.shape[0]
    )
    mean_rate = lax.axis_size("replica") ** (-0.5)
    mean_up = mean_up * mean_rate
    mean_down = mean_down * mean_rate
    mean_query = mean_query * mean_rate
    mean_key = mean_key * mean_rate
    mean_value = mean_value * mean_rate
    mean_mixed = mean_mixed * mean_rate
    mean_norm = mean_norm * mean_rate
    next_up = param_up - learn_rate * mean_up
    next_down = param_down - learn_rate * mean_down
    next_query = param_query - learn_rate * mean_query
    next_key = param_key - learn_rate * mean_key
    next_value = param_value - learn_rate * mean_value
    next_mixed = param_mixed - learn_rate * mean_mixed
    next_norm = param_norm - learn_rate * mean_norm
    half_up, half_down, half_query, half_key, half_value, half_mixed, half_norm = (
        lax.all_gather(next_up.astype(jnp.bfloat16), "replica", axis=0, tiled=True),
        lax.all_gather(next_down.astype(jnp.bfloat16), "replica", axis=1, tiled=True),
        lax.all_gather(next_query.astype(jnp.bfloat16), "replica", axis=0, tiled=True),
        lax.all_gather(next_key.astype(jnp.bfloat16), "replica", axis=0, tiled=True),
        lax.all_gather(next_value.astype(jnp.bfloat16), "replica", axis=0, tiled=True),
        lax.all_gather(next_mixed.astype(jnp.bfloat16), "replica", axis=1, tiled=True),
        lax.all_gather(next_norm.astype(jnp.bfloat16), "replica", axis=0, tiled=True),
    )
    return (
        half_up,
        half_down,
        half_query,
        half_key,
        half_value,
        half_mixed,
        half_norm,
        next_up,
        next_down,
        next_query,
        next_key,
        next_value,
        next_mixed,
        next_norm,
    )


def solution(mesh):
    placed = (
        P(("unit", "replica"), None, "model"),
        P(("unit", "replica"), "model", None),
        P(("unit", "replica"), None, "model"),
        P(("unit", "replica"), None, "model"),
        P(("unit", "replica"), None, "model"),
        P(("unit", "replica"), "model", None),
        P(("unit", "replica"), None),
        P(("unit", "replica"), "model"),
        P(("unit", "model"), "replica"),
        P(("unit", "replica"), "model"),
        P(("unit", "replica"), "model"),
        P(("unit", "replica"), "model"),
        P(("unit", "model"), "replica"),
        P(("unit", "replica")),
    )
    n = mesh.shape["replica"]
    return jax.shard_map(
        functools.partial(shards, n) if n == 2 else spread,
        mesh=mesh,
        in_specs=placed,
        out_specs=(
            P("unit", "model"),
            P(("unit", "model"), None),
            P("unit", "model"),
            P("unit", "model"),
            P("unit", "model"),
            P(("unit", "model"), None),
            P("unit"),
            P(("unit", "replica"), "model"),
            P(("unit", "model"), "replica"),
            P(("unit", "replica"), "model"),
            P(("unit", "replica"), "model"),
            P(("unit", "replica"), "model"),
            P(("unit", "model"), "replica"),
            P(("unit", "replica")),
        ),
        check_vma=False,
    )
```

```python
import functools

import jax
import jax.numpy as jnp
from jax import lax
from jax.experimental import pallas as pl
from jax.experimental.pallas import tpu as pltpu
from jax.sharding import PartitionSpec as P

learn_rate = 0.3
ANY = pl.BlockSpec(memory_space=pl.ANY)
VMEM_BYTES = 67043328


def pieces(shape, split_rows, parts):
    rows = shape[0]
    if rows % (16 * parts):
        parts = 1
    return [(part * (rows // parts), rows // parts) for part in range(parts)]


def plan(halves, by_row, small):
    chunks = []
    for at, half in enumerate(halves):
        parts = max(1, half[0] * half[1] // small)
        chunks += [(at, start, rows) for start, rows in pieces(half, by_row[at], parts)]
    return chunks


def exchange(n, by_row, chunks, rate, *refs):
    m = len(by_row)
    slopes, slope_norm = refs[:m], refs[m]
    params, param_norm = refs[m + 1 : 2 * m + 1], refs[2 * m + 1]
    refs = refs[2 * m + 2 :]
    halfs, norm_half = refs[:m], refs[m]
    kept, norm_next = refs[m + 1 : 2 * m + 1], refs[2 * m + 1]
    refs = refs[2 * m + 2 :]
    own, got = refs[:m], refs[m : 2 * m]
    (norms, norm_own, norm_got, norm_all, in_sem, keep_sem, send_sem, recv_sem,
     back_send, back_recv, norm_in, norm_send, norm_recv) = refs[2 * m :]

    me = lax.axis_index("replica")
    peer = 1 - me
    there = {"replica": peer}

    def half_of(at, who, start, rows):
        height, width = kept[at].shape
        if by_row[at]:
            return pl.ds(pl.multiple_of(who * height + start, 16), rows), pl.ds(0, width)
        return pl.ds(start, rows), pl.ds(pl.multiple_of(who * width, width), width)

    def remote(source, target, out_sem, in_sem):
        return pltpu.make_async_remote_copy(
            src_ref=source,
            dst_ref=target,
            send_sem=out_sem,
            recv_sem=in_sem,
            device_id=there,
            device_id_type=pl.DeviceIdType.MESH,
        )

    loads = []
    for c, (at, start, rows) in enumerate(chunks):
        mine = pl.ds(start, rows)
        loads.append((
            pltpu.make_async_copy(
                slopes[at].at[(0, *half_of(at, me, start, rows))], own[at].at[mine], in_sem.at[c]
            ),
            pltpu.make_async_copy(params[at].at[mine], kept[at].at[mine], keep_sem.at[c]),
        ))
    norm_loads = (
        pltpu.make_async_copy(slope_norm, norms.at[pl.ds(me, 1)], norm_in.at[0]),
        pltpu.make_async_copy(param_norm, norm_own, norm_in.at[1]),
    )

    barrier = pltpu.get_barrier_semaphore()
    pl.semaphore_signal(barrier, inc=1, device_id=there, device_id_type=pl.DeviceIdType.MESH)
    pl.semaphore_wait(barrier, 1)

    norm_sends = [
        remote(slope_norm, norms.at[pl.ds(me, 1)], norm_send.at[0], norm_recv.at[0]),
        remote(param_norm, norm_got, norm_send.at[1], norm_recv.at[1]),
    ]
    sends = [
        remote(
            slopes[at].at[(0, *half_of(at, peer, start, rows))],
            got[at].at[pl.ds(start, rows)],
            send_sem.at[c],
            recv_sem.at[c],
        )
        for c, (at, start, rows) in enumerate(chunks)
    ]
    for send in sends + norm_sends:
        send.start()
    for load in loads:
        load[0].start()
        load[1].start()
    for load in norm_loads:
        load.start()

    backs = []
    for c, (at, start, rows) in enumerate(chunks):
        loads[c][0].wait()
        loads[c][1].wait()
        sends[c].wait_recv()
        step = 32 if rows % 32 == 0 else 16
        height, width = kept[at].shape

        @pl.loop(0, rows // step)
        def update(block, at=at, start=start, step=step, height=height, width=width):
            first = pl.multiple_of(start + block * step, step)
            span = pl.ds(first, step)
            mean = (own[at][span] + got[at][span]) * rate
            moved = kept[at][span] - learn_rate * mean
            kept[at][span] = moved
            halfs[at][half_of(at, me, first, step)] = moved.astype(jnp.bfloat16)

        place = half_of(at, me, start, rows)
        back = remote(halfs[at].at[place], halfs[at].at[place], back_send.at[c], back_recv.at[c])
        back.start()
        backs.append(back)

    for load in norm_loads:
        load.wait()
    for send in norm_sends:
        send.wait_recv()
    width = norm_own.shape[0]
    total = norms[0:1] + norms[1:2]
    for where, held in ((me, norm_own), (peer, norm_got)):
        cut = pl.ds(pl.multiple_of(where * width, width), width)
        norm_all[0:1, cut] = held[...].reshape(1, width)
    moved = norm_all[...] - learn_rate * (total * rate)
    norm_all[...] = moved
    norm_half[...] = moved.reshape(n * width).astype(jnp.bfloat16)
    cut = pl.ds(pl.multiple_of(me * width, width), width)
    norm_next[...] = norm_all[0:1, cut].reshape(width)

    for send in sends + norm_sends:
        send.wait_send()
    for back in backs:
        back.wait()


def settle(count, *refs):
    sems = refs[-1]
    copies = [
        pltpu.make_async_copy(refs[k], refs[count + k], sems.at[k]) for k in range(count)
    ]
    for copy in copies:
        copy.start()
    for copy in copies:
        copy.wait()


def shards(n, *arrays):
    m = len(arrays) // 2 - 1
    slopes, slope_norm = list(arrays[:m]), arrays[m]
    params, param_norm = list(arrays[m + 1 : -1]), arrays[-1]
    turned = [2, 3, 4]
    by_row = [slope.shape[1] != param.shape[0] for slope, param in zip(slopes, params)]
    for at in turned:
        slopes[at] = slopes[at].transpose(0, 2, 1)
        params[at] = params[at].T
        by_row[at] = not by_row[at]
    f32, bf16 = jnp.float32, jnp.bfloat16
    halves = [param.shape for param in params]
    wholes = [slope.shape[1:] for slope in slopes]
    small = min(half[0] * half[1] for half in halves)
    chunks = plan(halves, by_row, small)
    count = len(chunks)
    width = param_norm.shape[0]
    dma = pltpu.SemaphoreType.DMA
    results = sum(rows * columns for rows, columns in wholes) * 2
    results += sum(rows * columns for rows, columns in halves) * 4
    outs = pl.pallas_call(
        functools.partial(exchange, n, by_row, chunks, n ** (-0.5)),
        out_shape=(
            *[pltpu.VMEM(whole, bf16) for whole in wholes],
            pltpu.VMEM((n * width,), bf16),
            *[pltpu.VMEM(half, f32) for half in halves],
            pltpu.VMEM((width,), f32),
        ),
        in_specs=[ANY] * (2 * m + 2),
        out_specs=[pl.BlockSpec(memory_space=pltpu.VMEM)] * (2 * m + 2),
        scratch_shapes=[
            *[pltpu.VMEM(half, f32) for half in halves * 2],
            pltpu.VMEM((n, n * width), f32),
            pltpu.VMEM((width,), f32),
            pltpu.VMEM((width,), f32),
            pltpu.VMEM((1, n * width), f32),
            *[dma((count,))] * 6,
            *[dma((2,))] * 3,
        ],
        compiler_params=pltpu.CompilerParams(
            collective_id=0, has_side_effects=True, vmem_limit_bytes=VMEM_BYTES - results - 192 * 1024
        ),
        name="exchange",
    )(*slopes, slope_norm, *params, param_norm)
    outs = list(pl.pallas_call(
        functools.partial(settle, len(outs)),
        out_shape=[jax.ShapeDtypeStruct(out.shape, out.dtype) for out in outs],
        in_specs=[pl.BlockSpec(memory_space=pltpu.VMEM)] * len(outs),
        out_specs=[ANY] * len(outs),
        scratch_shapes=[dma((len(outs),))],
        compiler_params=pltpu.CompilerParams(vmem_limit_bytes=2 * 1024 * 1024),
        name="settle",
    )(*outs))
    for at in turned:
        outs[at] = outs[at].T
        outs[m + 1 + at] = outs[m + 1 + at].T
    return tuple(outs)


def spread(
    slope_up,
    slope_down,
    slope_query,
    slope_key,
    slope_value,
    slope_mixed,
    slope_norm,
    param_up,
    param_down,
    param_query,
    param_key,
    param_value,
    param_mixed,
    param_norm,
):
    mean_up, mean_down, mean_query, mean_key, mean_value, mean_mixed = (
        lax.psum_scatter(slope_up[0], "replica", scatter_dimension=0, tiled=True),
        lax.psum_scatter(slope_down[0], "replica", scatter_dimension=1, tiled=True),
        lax.psum_scatter(slope_query[0], "replica", scatter_dimension=0, tiled=True),
        lax.psum_scatter(slope_key[0], "replica", scatter_dimension=0, tiled=True),
        lax.psum_scatter(slope_value[0], "replica", scatter_dimension=0, tiled=True),
        lax.psum_scatter(slope_mixed[0], "replica", scatter_dimension=1, tiled=True),
    )
    whole_norm = lax.psum(slope_norm[0], "replica")
    place = lax.axis_index("replica")
    mean_norm = lax.dynamic_slice_in_dim(
        whole_norm, place * param_norm.shape[0], param_norm.shape[0]
    )
    mean_rate = lax.axis_size("replica") ** (-0.5)
    mean_up = mean_up * mean_rate
    mean_down = mean_down * mean_rate
    mean_query = mean_query * mean_rate
    mean_key = mean_key * mean_rate
    mean_value = mean_value * mean_rate
    mean_mixed = mean_mixed * mean_rate
    mean_norm = mean_norm * mean_rate
    next_up = param_up - learn_rate * mean_up
    next_down = param_down - learn_rate * mean_down
    next_query = param_query - learn_rate * mean_query
    next_key = param_key - learn_rate * mean_key
    next_value = param_value - learn_rate * mean_value
    next_mixed = param_mixed - learn_rate * mean_mixed
    next_norm = param_norm - learn_rate * mean_norm
    half_up, half_down, half_query, half_key, half_value, half_mixed, half_norm = (
        lax.all_gather(next_up.astype(jnp.bfloat16), "replica", axis=0, tiled=True),
        lax.all_gather(next_down.astype(jnp.bfloat16), "replica", axis=1, tiled=True),
        lax.all_gather(next_query.astype(jnp.bfloat16), "replica", axis=0, tiled=True),
        lax.all_gather(next_key.astype(jnp.bfloat16), "replica", axis=0, tiled=True),
        lax.all_gather(next_value.astype(jnp.bfloat16), "replica", axis=0, tiled=True),
        lax.all_gather(next_mixed.astype(jnp.bfloat16), "replica", axis=1, tiled=True),
        lax.all_gather(next_norm.astype(jnp.bfloat16), "replica", axis=0, tiled=True),
    )
    return (
        half_up,
        half_down,
        half_query,
        half_key,
        half_value,
        half_mixed,
        half_norm,
        next_up,
        next_down,
        next_query,
        next_key,
        next_value,
        next_mixed,
        next_norm,
    )


def solution(mesh):
    placed = (
        P(("unit", "replica"), None, "model"),
        P(("unit", "replica"), "model", None),
        P(("unit", "replica"), None, "model"),
        P(("unit", "replica"), None, "model"),
        P(("unit", "replica"), None, "model"),
        P(("unit", "replica"), "model", None),
        P(("unit", "replica"), None),
        P(("unit", "replica"), "model"),
        P(("unit", "model"), "replica"),
        P(("unit", "replica"), "model"),
        P(("unit", "replica"), "model"),
        P(("unit", "replica"), "model"),
        P(("unit", "model"), "replica"),
        P(("unit", "replica")),
    )
    n = mesh.shape["replica"]
    return jax.shard_map(
        functools.partial(shards, n) if n == 2 else spread,
        mesh=mesh,
        in_specs=placed,
        out_specs=(
            P("unit", "model"),
            P(("unit", "model"), None),
            P("unit", "model"),
            P("unit", "model"),
            P("unit", "model"),
            P(("unit", "model"), None),
            P("unit"),
            P(("unit", "replica"), "model"),
            P(("unit", "model"), "replica"),
            P(("unit", "replica"), "model"),
            P(("unit", "replica"), "model"),
            P(("unit", "replica"), "model"),
            P(("unit", "model"), "replica"),
            P(("unit", "replica")),
        ),
        check_vma=False,
    )
```

```python
import functools

import jax
import jax.numpy as jnp
from jax import lax
from jax.experimental import pallas as pl
from jax.experimental.pallas import tpu as pltpu
from jax.sharding import PartitionSpec as P

learn_rate = 0.3
ANY = pl.BlockSpec(memory_space=pl.ANY)
VMEM_BYTES = 67043328


def pieces(shape, split_rows, parts):
    rows = shape[0]
    if rows % (16 * parts):
        parts = 1
    return [(part * (rows // parts), rows // parts) for part in range(parts)]


def plan(halves, by_row, small):
    chunks = []
    for at, half in enumerate(halves):
        parts = max(1, half[0] * half[1] // small)
        chunks += [(at, start, rows) for start, rows in pieces(half, by_row[at], parts)]
    return chunks


def exchange(n, by_row, chunks, rate, *refs):
    m = len(by_row)
    slopes, slope_norm = refs[:m], refs[m]
    params, param_norm = refs[m + 1 : 2 * m + 1], refs[2 * m + 1]
    refs = refs[2 * m + 2 :]
    halfs, norm_half = refs[:m], refs[m]
    kept, norm_next = refs[m + 1 : 2 * m + 1], refs[2 * m + 1]
    refs = refs[2 * m + 2 :]
    own, got = refs[:m], refs[m : 2 * m]
    (norms, norm_own, norm_got, norm_all, in_sem, keep_sem, send_sem, recv_sem,
     back_send, back_recv, norm_in, norm_send, norm_recv) = refs[2 * m :]

    me = lax.axis_index("replica")
    peer = 1 - me
    there = {"replica": peer}

    def half_of(at, who, start, rows):
        height, width = kept[at].shape
        if by_row[at]:
            return pl.ds(pl.multiple_of(who * height + start, 16), rows), pl.ds(0, width)
        return pl.ds(start, rows), pl.ds(pl.multiple_of(who * width, width), width)

    def remote(source, target, out_sem, in_sem):
        return pltpu.make_async_remote_copy(
            src_ref=source,
            dst_ref=target,
            send_sem=out_sem,
            recv_sem=in_sem,
            device_id=there,
            device_id_type=pl.DeviceIdType.MESH,
        )

    loads = []
    for c, (at, start, rows) in enumerate(chunks):
        mine = pl.ds(start, rows)
        loads.append((
            pltpu.make_async_copy(
                slopes[at].at[(0, *half_of(at, me, start, rows))], own[at].at[mine], in_sem.at[c]
            ),
            pltpu.make_async_copy(params[at].at[mine], kept[at].at[mine], keep_sem.at[c]),
        ))
    norm_loads = (
        pltpu.make_async_copy(slope_norm, norms.at[pl.ds(me, 1)], norm_in.at[0]),
        pltpu.make_async_copy(param_norm, norm_own, norm_in.at[1]),
    )

    barrier = pltpu.get_barrier_semaphore()
    pl.semaphore_signal(barrier, inc=1, device_id=there, device_id_type=pl.DeviceIdType.MESH)
    pl.semaphore_wait(barrier, 1)

    norm_sends = [
        remote(slope_norm, norms.at[pl.ds(me, 1)], norm_send.at[0], norm_recv.at[0]),
        remote(param_norm, norm_got, norm_send.at[1], norm_recv.at[1]),
    ]
    sends = [
        remote(
            slopes[at].at[(0, *half_of(at, peer, start, rows))],
            got[at].at[pl.ds(start, rows)],
            send_sem.at[c],
            recv_sem.at[c],
        )
        for c, (at, start, rows) in enumerate(chunks)
    ]
    for send in sends + norm_sends:
        send.start()
    for load in loads:
        load[0].start()
        load[1].start()
    for load in norm_loads:
        load.start()

    backs = []
    for c, (at, start, rows) in enumerate(chunks):
        loads[c][0].wait()
        loads[c][1].wait()
        sends[c].wait_recv()
        step = 32 if rows % 32 == 0 else 16
        height, width = kept[at].shape

        @pl.loop(0, rows // step)
        def update(block, at=at, start=start, step=step, height=height, width=width):
            first = pl.multiple_of(start + block * step, step)
            span = pl.ds(first, step)
            mean = (own[at][span] + got[at][span]) * rate
            moved = kept[at][span] - learn_rate * mean
            kept[at][span] = moved
            halfs[at][half_of(at, me, first, step)] = moved.astype(jnp.bfloat16)

        place = half_of(at, me, start, rows)
        back = remote(halfs[at].at[place], halfs[at].at[place], back_send.at[c], back_recv.at[c])
        back.start()
        backs.append(back)

    for load in norm_loads:
        load.wait()
    for send in norm_sends:
        send.wait_recv()
    width = norm_own.shape[0]
    total = norms[0:1] + norms[1:2]
    for where, held in ((me, norm_own), (peer, norm_got)):
        cut = pl.ds(pl.multiple_of(where * width, width), width)
        norm_all[0:1, cut] = held[...].reshape(1, width)
    moved = norm_all[...] - learn_rate * (total * rate)
    norm_all[...] = moved
    norm_half[...] = moved.reshape(n * width).astype(jnp.bfloat16)
    cut = pl.ds(pl.multiple_of(me * width, width), width)
    norm_next[...] = norm_all[0:1, cut].reshape(width)

    for send in sends + norm_sends:
        send.wait_send()
    for back in backs:
        back.wait()


def settle(count, *refs):
    sems = refs[-1]
    copies = [
        pltpu.make_async_copy(refs[k], refs[count + k], sems.at[k]) for k in range(count)
    ]
    for copy in copies:
        copy.start()
    for copy in copies:
        copy.wait()


def shards(n, *arrays):
    m = len(arrays) // 2 - 1
    slopes, slope_norm = list(arrays[:m]), arrays[m]
    params, param_norm = list(arrays[m + 1 : -1]), arrays[-1]
    turned = [2, 3, 4]
    by_row = [slope.shape[1] != param.shape[0] for slope, param in zip(slopes, params)]
    for at in turned:
        slopes[at] = slopes[at].transpose(0, 2, 1)
        params[at] = params[at].T
        by_row[at] = not by_row[at]
    f32, bf16 = jnp.float32, jnp.bfloat16
    halves = [param.shape for param in params]
    wholes = [slope.shape[1:] for slope in slopes]
    small = min(half[0] * half[1] for half in halves)
    chunks = plan(halves, by_row, 4 * small)
    count = len(chunks)
    width = param_norm.shape[0]
    dma = pltpu.SemaphoreType.DMA
    results = sum(rows * columns for rows, columns in wholes) * 2
    results += sum(rows * columns for rows, columns in halves) * 4
    outs = pl.pallas_call(
        functools.partial(exchange, n, by_row, chunks, n ** (-0.5)),
        out_shape=(
            *[pltpu.VMEM(whole, bf16) for whole in wholes],
            pltpu.VMEM((n * width,), bf16),
            *[pltpu.VMEM(half, f32) for half in halves],
            pltpu.VMEM((width,), f32),
        ),
        in_specs=[ANY] * (2 * m + 2),
        out_specs=[pl.BlockSpec(memory_space=pltpu.VMEM)] * (2 * m + 2),
        scratch_shapes=[
            *[pltpu.VMEM(half, f32) for half in halves * 2],
            pltpu.VMEM((n, n * width), f32),
            pltpu.VMEM((width,), f32),
            pltpu.VMEM((width,), f32),
            pltpu.VMEM((1, n * width), f32),
            *[dma((count,))] * 6,
            *[dma((2,))] * 3,
        ],
        compiler_params=pltpu.CompilerParams(
            collective_id=0, has_side_effects=True, vmem_limit_bytes=VMEM_BYTES - results - 192 * 1024
        ),
        name="exchange",
    )(*slopes, slope_norm, *params, param_norm)
    outs = list(pl.pallas_call(
        functools.partial(settle, len(outs)),
        out_shape=[jax.ShapeDtypeStruct(out.shape, out.dtype) for out in outs],
        in_specs=[pl.BlockSpec(memory_space=pltpu.VMEM)] * len(outs),
        out_specs=[ANY] * len(outs),
        scratch_shapes=[dma((len(outs),))],
        compiler_params=pltpu.CompilerParams(vmem_limit_bytes=2 * 1024 * 1024),
        name="settle",
    )(*outs))
    for at in turned:
        outs[at] = outs[at].T
        outs[m + 1 + at] = outs[m + 1 + at].T
    return tuple(outs)


def spread(
    slope_up,
    slope_down,
    slope_query,
    slope_key,
    slope_value,
    slope_mixed,
    slope_norm,
    param_up,
    param_down,
    param_query,
    param_key,
    param_value,
    param_mixed,
    param_norm,
):
    mean_up, mean_down, mean_query, mean_key, mean_value, mean_mixed = (
        lax.psum_scatter(slope_up[0], "replica", scatter_dimension=0, tiled=True),
        lax.psum_scatter(slope_down[0], "replica", scatter_dimension=1, tiled=True),
        lax.psum_scatter(slope_query[0], "replica", scatter_dimension=0, tiled=True),
        lax.psum_scatter(slope_key[0], "replica", scatter_dimension=0, tiled=True),
        lax.psum_scatter(slope_value[0], "replica", scatter_dimension=0, tiled=True),
        lax.psum_scatter(slope_mixed[0], "replica", scatter_dimension=1, tiled=True),
    )
    whole_norm = lax.psum(slope_norm[0], "replica")
    place = lax.axis_index("replica")
    mean_norm = lax.dynamic_slice_in_dim(
        whole_norm, place * param_norm.shape[0], param_norm.shape[0]
    )
    mean_rate = lax.axis_size("replica") ** (-0.5)
    mean_up = mean_up * mean_rate
    mean_down = mean_down * mean_rate
    mean_query = mean_query * mean_rate
    mean_key = mean_key * mean_rate
    mean_value = mean_value * mean_rate
    mean_mixed = mean_mixed * mean_rate
    mean_norm = mean_norm * mean_rate
    next_up = param_up - learn_rate * mean_up
    next_down = param_down - learn_rate * mean_down
    next_query = param_query - learn_rate * mean_query
    next_key = param_key - learn_rate * mean_key
    next_value = param_value - learn_rate * mean_value
    next_mixed = param_mixed - learn_rate * mean_mixed
    next_norm = param_norm - learn_rate * mean_norm
    half_up, half_down, half_query, half_key, half_value, half_mixed, half_norm = (
        lax.all_gather(next_up.astype(jnp.bfloat16), "replica", axis=0, tiled=True),
        lax.all_gather(next_down.astype(jnp.bfloat16), "replica", axis=1, tiled=True),
        lax.all_gather(next_query.astype(jnp.bfloat16), "replica", axis=0, tiled=True),
        lax.all_gather(next_key.astype(jnp.bfloat16), "replica", axis=0, tiled=True),
        lax.all_gather(next_value.astype(jnp.bfloat16), "replica", axis=0, tiled=True),
        lax.all_gather(next_mixed.astype(jnp.bfloat16), "replica", axis=1, tiled=True),
        lax.all_gather(next_norm.astype(jnp.bfloat16), "replica", axis=0, tiled=True),
    )
    return (
        half_up,
        half_down,
        half_query,
        half_key,
        half_value,
        half_mixed,
        half_norm,
        next_up,
        next_down,
        next_query,
        next_key,
        next_value,
        next_mixed,
        next_norm,
    )


def solution(mesh):
    placed = (
        P(("unit", "replica"), None, "model"),
        P(("unit", "replica"), "model", None),
        P(("unit", "replica"), None, "model"),
        P(("unit", "replica"), None, "model"),
        P(("unit", "replica"), None, "model"),
        P(("unit", "replica"), "model", None),
        P(("unit", "replica"), None),
        P(("unit", "replica"), "model"),
        P(("unit", "model"), "replica"),
        P(("unit", "replica"), "model"),
        P(("unit", "replica"), "model"),
        P(("unit", "replica"), "model"),
        P(("unit", "model"), "replica"),
        P(("unit", "replica")),
    )
    n = mesh.shape["replica"]
    return jax.shard_map(
        functools.partial(shards, n) if n == 2 else spread,
        mesh=mesh,
        in_specs=placed,
        out_specs=(
            P("unit", "model"),
            P(("unit", "model"), None),
            P("unit", "model"),
            P("unit", "model"),
            P("unit", "model"),
            P(("unit", "model"), None),
            P("unit"),
            P(("unit", "replica"), "model"),
            P(("unit", "model"), "replica"),
            P(("unit", "replica"), "model"),
            P(("unit", "replica"), "model"),
            P(("unit", "replica"), "model"),
            P(("unit", "model"), "replica"),
            P(("unit", "replica")),
        ),
        check_vma=False,
    )
```
